32 devices in a mesh: lat: 8 (over z, y), ch: 4 (over x, core).
Axes of the slice: x: 2, y: 2, z: 4, core: 2. Of those that a mesh axis runs over, the one named last changes fastest.
Arguments:
- state: float32 [1, 24, 180, 768], P(None, 'lat', None, 'ch'), may hold values from -30 to 30
- norm_gains: bfloat16 [2, 768], P(None, 'ch'), may hold values from 0.099609375 to 1.8984375
- channel_biases: bfloat16 [3, 768], P(None, 'ch'), may hold values from -2 to 2
- filter_in: float32 [2, 8, 96, 96], P(None, 'ch'), may hold values from -0.4375 to 0.4375
- filter_in_bias: float32 [2, 8, 96], P(None, 'ch'), may hold values from -2 to 2
- filter_out: float32 [2, 8, 96, 96], P(None, 'ch'), may hold values from -0.4375 to 0.4375
- filter_out_bias: float32 [2, 8, 96], P(None, 'ch'), may hold values from -2 to 2
- up_weight: bfloat16 [768, 3072], P(None, 'ch'), may hold values from -0.21875 to 0.21875
- up_bias: bfloat16 [3072], P('ch'), may hold values from -2 to 2
- down_weight: bfloat16 [3072, 768], P('ch'), may hold values from -0.109375 to 0.109375
Outputs:
- final_state: float32 [1, 24, 180, 768], P(None, 'lat', None, 'ch')
The draws below stay inside these ranges and needn't reach their ends.
All inputs are finite; a program needn't handle non-finite values.
Results may differ from the reference program's by a relative error of at most 0.0012.
Values may be sent and summed in bfloat16 or wider, within the bound.
A program may use at most 128 MiB of HBM per device.

```python
import math
import jax
import jax.numpy as jnp
from jax import lax

D = 768
FF = 3072
W = 180
NB = 8
M = 64
STEPS = 4
B = 1
H = 24
BS = 96


def draw_state(key, part):
    subkeys = jax.random.split(key, 3)
    channel_pos = jnp.arange(D).astype(jnp.float32) / D
    column_scale = 0.3 * jnp.exp(jax.random.uniform(subkeys[0], (D,), jnp.float32) * math.log(10.0)) * jnp.exp(channel_pos * 0.5 * math.log(3.0))
    channel_shift = 0.2 + 0.6 * channel_pos + 0.3 * jax.random.normal(subkeys[1], (D,), jnp.float32)
    value = jax.random.normal(subkeys[2], (B, H, W, D), jnp.float32) * column_scale + channel_shift
    return jnp.clip(value, -30.0, 30.0)


def block_scale(own_key, shape, cuts, smallest, high):
    level = 1.0
    for dim, shards_of in cuts:
        steps = jax.random.uniform(jax.random.fold_in(jax.random.fold_in(own_key, 6), dim), (shards_of,), jnp.float32, smallest / len(cuts), high / len(cuts))
        level = level * jnp.repeat(jnp.exp(steps), shape[dim] // shards_of).reshape((-1,) + (1,) * (len(shape) - 1 - dim))
    return level


def scatter_about(own_key, dims, scale, most, cuts=(), kind=jnp.bfloat16):
    values = scale * jax.random.normal(own_key, dims, jnp.float32)
    if cuts:
        values = values * block_scale(own_key, dims, cuts, -0.22, 0.18)
    return jnp.clip(values, -most, most).astype(kind)


def setup_inputs(seed: int = 0) -> dict:
    key_list = jax.random.split(jax.random.key(seed), 11)
    state = draw_state(jax.random.fold_in(key_list[10], 71), 0)
    norm_gains = jnp.clip(1.0 + 0.18 * jax.random.normal(key_list[1], (2, D), jnp.float32), 0.099609375, 1.8984375).astype(jnp.bfloat16)
    channel_biases = scatter_about(key_list[2], (3, D), 0.3, 2.0, ((1, 4),))
    filter_in = scatter_about(key_list[3], (2, NB, BS, BS), (2 * BS) ** -0.5, 0.4375, ((1, 4),), jnp.float32)
    filter_in_bias = scatter_about(key_list[4], (2, NB, BS), 0.3, 2.0, ((1, 4),), jnp.float32)
    filter_out = scatter_about(key_list[5], (2, NB, BS, BS), (2 * BS) ** -0.5, 0.4375, ((1, 4),), jnp.float32)
    filter_out_bias = scatter_about(key_list[6], (2, NB, BS), 0.3, 2.0, ((1, 4),), jnp.float32)
    up_weight = scatter_about(key_list[7], (D, FF), D ** -0.5, 0.21875, ((1, 4),))
    up_bias = scatter_about(key_list[8], (FF,), 0.3, 2.0, ((0, 4),))
    down_weight = scatter_about(key_list[9], (FF, D), FF ** -0.5, 0.109375, ((0, 4),))
    return dict(state=state, norm_gains=norm_gains, channel_biases=channel_biases, filter_in=filter_in, filter_in_bias=filter_in_bias, filter_out=filter_out, filter_out_bias=filter_out_bias, up_weight=up_weight, up_bias=up_bias, down_weight=down_weight)


EPS = 1e-05
SHRINK = 0.01
HIGH = lax.Precision.HIGHEST

def longitude_tables(width, modes):
    column = jnp.arange(width, dtype=jnp.int32)[:, None]
    order = jnp.arange(modes, dtype=jnp.int32)[None, :]
    angle = 2.0 * math.pi / width * (column * order % width).astype(jnp.float32)
    doubled = jnp.where(order == 0, 1.0, 2.0).astype(jnp.float32)
    return (jnp.cos(angle), jnp.sin(angle), jnp.cos(angle) * doubled, jnp.sin(angle) * doubled)

def latitude_tables(height):
    column = jnp.arange(height, dtype=jnp.int32)[:, None]
    order = jnp.arange(height, dtype=jnp.int32)[None, :]
    angle = 2.0 * math.pi / height * (column * order % height).astype(jnp.float32)
    return (jnp.cos(angle), jnp.sin(angle))

def layer_norm(values, gain, shift):
    mean = lax.optimization_barrier(jnp.sum(values, -1, keepdims=True)) / values.shape[-1]
    spread = lax.optimization_barrier(jnp.sum(values * values, -1, keepdims=True)) / values.shape[-1] - mean * mean
    return (values - mean) * lax.rsqrt(spread + EPS) * gain + shift

def soft_shrink(values):
    return jnp.where(values > SHRINK, values - SHRINK, jnp.where(values < -SHRINK, values + SHRINK, 0.0))

def block_apply(left, matrix):
    return jnp.einsum('bkmnj,nji->bkmni', left, matrix, precision=HIGH)

def spectral_mlp(real_part, imag_part, filter_in, filter_in_bias, filter_out, filter_out_bias):
    shape = real_part.shape
    blocks = filter_in.shape[1]
    size = filter_in.shape[2]
    real_blocks = real_part.reshape(shape[:-1] + (blocks, size))
    imag_blocks = imag_part.reshape(shape[:-1] + (blocks, size))
    first_real = jax.nn.relu(block_apply(real_blocks, filter_in[0]) - block_apply(imag_blocks, filter_in[1]) + filter_in_bias[0])
    first_imag = jax.nn.relu(block_apply(imag_blocks, filter_in[0]) + block_apply(real_blocks, filter_in[1]) + filter_in_bias[1])
    second_real = block_apply(first_real, filter_out[0]) - block_apply(first_imag, filter_out[1]) + filter_out_bias[0]
    second_imag = block_apply(first_imag, filter_out[0]) + block_apply(first_real, filter_out[1]) + filter_out_bias[1]
    return (soft_shrink(second_real).reshape(shape), soft_shrink(second_imag).reshape(shape))

def spectral_filter(normed, filter_in, filter_in_bias, filter_out, filter_out_bias):
    height = normed.shape[1]
    width = normed.shape[2]
    lon_cos, lon_sin, back_cos, back_sin = longitude_tables(width, M)
    lat_cos, lat_sin = latitude_tables(height)
    scale = 1.0 / math.sqrt(height * width)
    real_lon = jnp.einsum('bhwd,wm->bhmd', normed, lon_cos, precision=HIGH)
    imag_lon = -jnp.einsum('bhwd,wm->bhmd', normed, lon_sin, precision=HIGH)
    real_spec = (jnp.einsum('kh,bhmd->bkmd', lat_cos, real_lon, precision=HIGH) + jnp.einsum('kh,bhmd->bkmd', lat_sin, imag_lon, precision=HIGH)) * scale
    imag_spec = (jnp.einsum('kh,bhmd->bkmd', lat_cos, imag_lon, precision=HIGH) - jnp.einsum('kh,bhmd->bkmd', lat_sin, real_lon, precision=HIGH)) * scale
    out_real, out_imag = spectral_mlp(real_spec, imag_spec, filter_in, filter_in_bias, filter_out, filter_out_bias)
    real_rows = jnp.einsum('kh,bkmd->bhmd', lat_cos, out_real, precision=HIGH) - jnp.einsum('kh,bkmd->bhmd', lat_sin, out_imag, precision=HIGH)
    imag_rows = jnp.einsum('kh,bkmd->bhmd', lat_cos, out_imag, precision=HIGH) + jnp.einsum('kh,bkmd->bhmd', lat_sin, out_real, precision=HIGH)
    back = jnp.einsum('bhmd,wm->bhwd', real_rows, back_cos, precision=HIGH) - jnp.einsum('bhmd,wm->bhwd', imag_rows, back_sin, precision=HIGH)
    return back * scale

def reference(state, norm_gains, channel_biases, filter_in, filter_in_bias, filter_out, filter_out_bias, up_weight, up_bias, down_weight):
    gains = norm_gains.astype(jnp.float32)
    shifts = channel_biases.astype(jnp.float32)
    values = state
    for step_index in range(STEPS):
        normed = layer_norm(values, gains[0], shifts[0])
        values = values + spectral_filter(normed, filter_in, filter_in_bias, filter_out, filter_out_bias) + normed
        normed_two = layer_norm(values, gains[1], shifts[1]).astype(jnp.bfloat16)
        flat = normed_two.reshape(-1, normed_two.shape[-1])
        pre = jnp.dot(flat, up_weight, preferred_element_type=jnp.float32) + up_bias.astype(jnp.float32)
        hidden = jax.nn.gelu(pre, approximate=False).astype(jnp.bfloat16)
        mixed = jnp.dot(hidden, down_weight, preferred_element_type=jnp.float32) + shifts[2]
        values = values + mixed.reshape(values.shape)
    return values
```

```python
import functools
import math

import jax
import jax.numpy as jnp
from jax import lax
import numpy as np
from jax.experimental import pallas as pl
from jax.experimental.pallas import tpu as pltpu
from jax.sharding import PartitionSpec as P

D = 768
M = 64
STEPS = 4


EPS = 1e-05
SHRINK = 0.01
HIGH = lax.Precision.HIGHEST


def longitude_tables(width, modes):
    column = jnp.arange(width, dtype=jnp.int32)[:, None]
    order = jnp.arange(modes, dtype=jnp.int32)[None, :]
    angle = 2.0 * math.pi / width * (column * order % width).astype(jnp.float32)
    doubled = jnp.where(order == 0, 1.0, 2.0).astype(jnp.float32)
    return (jnp.cos(angle), jnp.sin(angle), jnp.cos(angle) * doubled, jnp.sin(angle) * doubled)


def latitude_tables(height):
    column = jnp.arange(height, dtype=jnp.int32)[:, None]
    order = jnp.arange(height, dtype=jnp.int32)[None, :]
    angle = 2.0 * math.pi / height * (column * order % height).astype(jnp.float32)
    return (jnp.cos(angle), jnp.sin(angle))


def layer_norm(values, gain, shift):
    mean = jnp.sum(values, -1, keepdims=True) / values.shape[-1]
    spread = jnp.sum(values * values, -1, keepdims=True) / values.shape[-1] - mean * mean
    return (values - mean) * lax.rsqrt(spread + EPS) * gain + shift


def soft_shrink(values):
    return jnp.where(
        values > SHRINK, values - SHRINK, jnp.where(values < -SHRINK, values + SHRINK, 0.0)
    )


def block_apply(left, matrix):
    return jnp.einsum("bkmnj,nji->bkmni", left, matrix, precision=HIGH)


def spectral_mlp(real_part, imag_part, filter_in, filter_in_bias, filter_out, filter_out_bias):
    shape = real_part.shape
    blocks = filter_in.shape[1]
    size = filter_in.shape[2]
    real_blocks = real_part.reshape(shape[:-1] + (blocks, size))
    imag_blocks = imag_part.reshape(shape[:-1] + (blocks, size))
    first_real = jax.nn.relu(
        block_apply(real_blocks, filter_in[0])
        - block_apply(imag_blocks, filter_in[1])
        + filter_in_bias[0]
    )
    first_imag = jax.nn.relu(
        block_apply(imag_blocks, filter_in[0])
        + block_apply(real_blocks, filter_in[1])
        + filter_in_bias[1]
    )
    second_real = (
        block_apply(first_real, filter_out[0])
        - block_apply(first_imag, filter_out[1])
        + filter_out_bias[0]
    )
    second_imag = (
        block_apply(first_imag, filter_out[0])
        + block_apply(first_real, filter_out[1])
        + filter_out_bias[1]
    )
    return (soft_shrink(second_real).reshape(shape), soft_shrink(second_imag).reshape(shape))


def local(
    state,
    norm_gains,
    channel_biases,
    filter_in,
    filter_in_bias,
    filter_out,
    filter_out_bias,
    up_weight,
    up_bias,
    down_weight,
):
    width = state.shape[2]
    height = state.shape[1] * lax.axis_size("lat")
    scale = 1.0 / math.sqrt(height * width)
    lon_cos, lon_sin, back_cos, back_sin = longitude_tables(width, M)
    lat_cos, lat_sin = latitude_tables(height)
    gains = norm_gains.astype(jnp.float32)
    shifts = channel_biases.astype(jnp.float32)
    full_up, full_gains, full_biases = (
        lax.all_gather(up_weight, "ch", axis=1, tiled=True),
        lax.all_gather(norm_gains, "ch", axis=1, tiled=True),
        lax.all_gather(channel_biases, "ch", axis=1, tiled=True),
    )
    full_down, full_up_bias = (
        lax.all_gather(down_weight, "ch", axis=0, tiled=True),
        lax.all_gather(up_bias, "ch", axis=0, tiled=True),
    )
    wide_gains = full_gains.astype(jnp.float32)
    wide_biases = full_biases.astype(jnp.float32)
    wide_up_bias = full_up_bias.astype(jnp.float32)
    values = state
    for step_index in range(STEPS):
        total, squares = lax.psum(
            (jnp.sum(values, -1, keepdims=True), jnp.sum(values * values, -1, keepdims=True)), "ch"
        )
        mean = total / D
        mean, spread = (mean, squares / D - mean * mean)
        normed = (values - mean) * lax.rsqrt(spread + EPS) * gains[0] + shifts[0]
        real_lon = jnp.einsum("bhwd,wm->bhmd", normed, lon_cos, precision=HIGH)
        imag_lon = -jnp.einsum("bhwd,wm->bhmd", normed, lon_sin, precision=HIGH)
        stacked = lax.all_to_all(
            jnp.stack((real_lon, imag_lon)), "lat", split_axis=3, concat_axis=2, tiled=True
        )
        spectral_real_lon = stacked[0]
        spectral_imag_lon = stacked[1]
        real_spec = (
            jnp.einsum("kh,bhmd->bkmd", lat_cos, spectral_real_lon, precision=HIGH)
            + jnp.einsum("kh,bhmd->bkmd", lat_sin, spectral_imag_lon, precision=HIGH)
        ) * scale
        imag_spec = (
            jnp.einsum("kh,bhmd->bkmd", lat_cos, spectral_imag_lon, precision=HIGH)
            - jnp.einsum("kh,bhmd->bkmd", lat_sin, spectral_real_lon, precision=HIGH)
        ) * scale
        out_real, out_imag = spectral_mlp(
            real_spec, imag_spec, filter_in, filter_in_bias, filter_out, filter_out_bias
        )
        real_rows = jnp.einsum("kh,bkmd->bhmd", lat_cos, out_real, precision=HIGH) - jnp.einsum(
            "kh,bkmd->bhmd", lat_sin, out_imag, precision=HIGH
        )
        imag_rows = jnp.einsum("kh,bkmd->bhmd", lat_cos, out_imag, precision=HIGH) + jnp.einsum(
            "kh,bkmd->bhmd", lat_sin, out_real, precision=HIGH
        )
        rows = lax.all_to_all(
            jnp.stack((real_rows, imag_rows)), "lat", split_axis=2, concat_axis=3, tiled=True
        )
        back = jnp.einsum("bhmd,wm->bhwd", rows[0], back_cos, precision=HIGH) - jnp.einsum(
            "bhmd,wm->bhwd", rows[1], back_sin, precision=HIGH
        )
        values = values + back * scale + normed
        owned = lax.all_to_all(values, "ch", split_axis=2, concat_axis=3, tiled=True)
        normed_two = layer_norm(owned, wide_gains[1], wide_biases[1]).astype(jnp.bfloat16)
        flat = normed_two.reshape(-1, normed_two.shape[-1])
        pre = jnp.dot(flat, full_up, preferred_element_type=jnp.float32) + wide_up_bias
        hidden = jax.nn.gelu(pre, approximate=False).astype(jnp.bfloat16)
        mixed = jnp.dot(hidden, full_down, preferred_element_type=jnp.float32) + wide_biases[2]
        values = values + lax.all_to_all(
            mixed.reshape(owned.shape), "ch", split_axis=3, concat_axis=2, tiled=True
        )
    return values


PIECES = 2
F32 = jnp.float32
BF16 = jnp.bfloat16
MESH = pl.DeviceIdType.MESH


def split_table(table):
    high = np.asarray(table, np.float32).astype(jnp.bfloat16)
    low = (table - high.astype(np.float64)).astype(np.float32).astype(jnp.bfloat16)
    return np.stack((high, low))


def fourier_tables(width, padded, height, modes, owners):
    scale = 1.0 / math.sqrt(height * width)
    share = modes // owners
    order = np.arange(modes).reshape(owners, share)
    angle = 2.0 * np.pi / width * (order[:, :, None] * np.arange(width) % width)
    forward = np.zeros((owners, 2, share, padded))
    forward[:, 0, :, :width] = np.cos(angle)
    forward[:, 1, :, :width] = -np.sin(angle)
    doubled = np.where(order == 0, 1.0, 2.0)[:, None, :, None] * scale
    backward = (forward * doubled).reshape(2 * modes, padded).T
    forward = forward.reshape(2 * modes, padded)
    rows = np.arange(height)
    turn = 2.0 * np.pi / height * (rows[:, None] * rows[None, :] % height)
    cos, sin, eye = np.cos(turn), np.sin(turn), np.eye(share)
    mix = np.array([[cos, sin], [-sin, cos]])
    size = 2 * height * share
    lat = np.einsum("abkh,mn->akmhbn", mix, eye).reshape(size, size) * scale
    unmix = np.array([[cos, -sin], [sin, cos]])
    back = np.einsum("bahk,mn->hbmakn", unmix, eye).reshape(size, size)
    return tuple(split_table(t) for t in (forward, lat, back, backward))


def dot(left, right):
    return jnp.dot(left, right, preferred_element_type=F32)


def halves(values):
    high = values.astype(BF16)
    return high, (values - high.astype(F32)).astype(BF16)


def gelu(values):
    return 0.5 * values * (1.0 + lax.erf(values * (1.0 / math.sqrt(2.0))))


def rollout(
    lats,
    chans,
    state,
    gains,
    shifts,
    fin,
    fin_bias,
    fout,
    fout_bias,
    up,
    up_bias,
    down,
    t_lon,
    t_lat,
    t_rows,
    t_back,
    out,
    x,
    stat_send,
    stat_recv,
    lon_send,
    lon_recv,
    row_send,
    row_recv,
    tok_send,
    tok_recv,
    mix_send,
    mix_recv,
    bias_send,
    bias_recv,
    up_recv,
    down_recv,
    partial,
    hidden,
    mixing,
    send_sem,
    recv_sem,
):
    lat, ch = lax.axis_index("lat"), lax.axis_index("ch")
    core = lax.rem(ch, 2)
    partner = ch + 1 - 2 * core
    rows, width, own = state.shape
    padded = x.shape[0] // rows
    half = x.shape[0] // 2
    piece = half // PIECES
    modes = t_lon.shape[1]
    wide = chans * own
    hid = up.shape[-1]

    def lat_peer(k):
        return lax.rem(lat + k, lats)

    def ch_peer(k):
        return lax.rem((partner if k % 2 else ch) + k - k % 2, chans)

    def ch_source(k):
        return lax.rem((partner if k % 2 else ch) + chans - (k - k % 2), chans)

    def half_of(k):
        return 1 - core if k % 2 else core

    far_first = tuple(range(2, chans)) + (1,)

    barrier = pltpu.get_barrier_semaphore()
    for k in range(1, lats):
        pl.semaphore_signal(barrier, inc=1, device_id={"lat": lat_peer(k)}, device_id_type=MESH)
    for k in range(1, chans):
        pl.semaphore_signal(barrier, inc=1, device_id={"ch": ch_peer(k)}, device_id_type=MESH)

    def copy(kind, k, source, target, device):
        return pltpu.make_async_remote_copy(
            src_ref=source,
            dst_ref=target,
            send_sem=send_sem.at[kind, k],
            recv_sem=recv_sem.at[kind, k],
            device_id=device,
            device_id_type=MESH,
        )

    gain = gains[...].astype(F32)
    shift = shifts[...].astype(F32)
    bias_send[...] = jnp.broadcast_to(up_bias[...].astype(F32), bias_send.shape)
    x[...] = jnp.zeros_like(x)
    for r in range(rows):
        x[r * padded : r * padded + width] = state[r]
    for layer, weights in enumerate((fin, fout)):
        for i in range(2):
            mixing[layer, i, 0], mixing[layer, i, 1] = halves(weights[i])
    pl.semaphore_wait(barrier, lats + chans - 2)
    setup = [
        copy(2, 0, bias_send, bias_recv, {"ch": partner}),
        copy(3, 0, up, up_recv, {"ch": partner}),
        copy(4, 0, down, down_recv, {"ch": partner}),
    ]
    lane = lax.broadcasted_iota(jnp.int32, (x.shape[0], 128), 1)

    def start(copies):
        for each in copies:
            each.start()
        return copies

    def finish(copies):
        for each in copies:
            each.wait()

    def norm_terms(kind, extra):
        values = x[...]
        total = jnp.sum(values, -1, keepdims=True)
        squares = jnp.sum(values * values, -1, keepdims=True)
        packed = jnp.where(lane == 0, total, jnp.where(lane == 1, squares, 0.0))
        stat_send[kind] = jnp.transpose(packed)[0:8]
        copies = start(
            [
                copy(kind, lats + k, stat_send.at[kind], stat_recv.at[kind, k], {"ch": ch_peer(k)})
                for k in range(1, chans)
            ]
        )
        start(extra)
        finish(copies)
        total = stat_send[kind]
        for k in range(1, chans):
            total = total + stat_recv[kind, k]
        total = jnp.transpose(total)
        mean = total[:, 0:1] / wide
        return mean, lax.rsqrt(total[:, 1:2] / wide - mean * mean + EPS)

    def step(first):
        mean, scaled = norm_terms(0, setup if first else [])
        for r in range(rows):
            part = slice(r * padded, (r + 1) * padded)
            now = x[part]
            normed = (now - mean[part]) * scaled[part] * gain[0:1] + shift[0:1]
            x[part] = now + normed
            high, low = halves(normed)
            spectra = dot(t_lon[0], high) + dot(t_lon[0], low) + dot(t_lon[1], high)
            lon_send[:, r] = spectra.astype(BF16).reshape(lats, modes // lats, own)
        copies = start(
            [
                copy(0, k, lon_send.at[lat_peer(k)], lon_recv.at[lat], {"lat": lat_peer(k)})
                for k in range(1, lats)
            ]
        )
        lon_recv[pl.ds(lat, 1)] = lon_send[pl.ds(lat, 1)]
        finish(copies)
        data = lon_recv[...].reshape(-1, own)
        spec = dot(t_lat[0], data) + dot(t_lat[1], data)
        split = spec.shape[0] // 2

        def complex_apply(pair, layer, bias):
            high, low = halves(pair)
            one, two = (
                dot(high, mixing[layer, i, 0])
                + dot(low, mixing[layer, i, 0])
                + dot(high, mixing[layer, i, 1])
                for i in range(2)
            )
            return (one[:split] - two[split:] + bias[0:1], one[split:] + two[:split] + bias[1:2])

        real, imag = complex_apply(spec, 0, fin_bias)
        pair = jnp.concatenate((jnp.maximum(real, 0.0), jnp.maximum(imag, 0.0)), 0)
        real, imag = complex_apply(pair, 1, fout_bias)
        high, low = halves(jnp.concatenate((soft_shrink(real), soft_shrink(imag)), 0))
        back = dot(t_rows[0], high) + dot(t_rows[0], low) + dot(t_rows[1], high)
        row_send[...] = back.astype(BF16).reshape(row_send.shape)
        copies = start(
            [
                copy(1, k, row_send.at[lat_peer(k)], row_recv.at[lat], {"lat": lat_peer(k)})
                for k in range(1, lats)
            ]
        )
        row_recv[pl.ds(lat, 1)] = row_send[pl.ds(lat, 1)]
        finish(copies)
        for r in range(rows):
            part = slice(r * padded, (r + 1) * padded)
            data = row_recv[:, r].reshape(-1, own)
            x[part] = x[part] + dot(t_back[0], data) + dot(t_back[1], data)
        mean, scaled = norm_terms(1, [])
        for p in range(PIECES):
            for h in range(2):
                part = slice(h * half + p * piece, h * half + (p + 1) * piece)
                normed = (x[part] - mean[part]) * scaled[part] * gain[1:2] + shift[1:2]
                tok_send[h, p] = normed.astype(BF16)
        tokens = [
            {
                k: copy(
                    5 + p, k, tok_send.at[half_of(k), p], tok_recv.at[p, k], {"ch": ch_peer(k)}
                )
                for k in far_first
            }
            for p in range(PIECES)
        ]
        for p in range(PIECES):
            start(tokens[p].values())
        if first:
            finish(setup)
        results = []
        chunk = 256
        blocks = [(s, lo) for s in range(2) for lo in range(0, hid, chunk)]
        for p in range(PIECES):
            tok_recv[p, 0] = tok_send[core, p]
            tokens[p][1].wait_recv()
            for s, lo in blocks:
                weight, bias = ((up, bias_send), (up_recv, bias_recv))[s]
                cut = slice(lo, lo + chunk)
                pre = bias[0:1, cut]
                for k in range(2):
                    pre = pre + dot(tok_recv[p, k], weight[ch_source(k), :, cut])
                partial[s, :, cut] = pre
            for k in range(2, chans):
                tokens[p][k].wait_recv()
            for s, lo in blocks:
                weight = (up, up_recv)[s]
                cut = slice(lo, lo + chunk)
                pre = partial[s, :, cut]
                for k in range(2, chans):
                    pre = pre + dot(tok_recv[p, k], weight[ch_source(k), :, cut])
                hidden[s, :, cut] = gelu(pre).astype(BF16)
            for k in far_first + (0,):
                peer = ch_peer(k)
                mixed = dot(hidden[0], down[peer]) + dot(hidden[1], down_recv[peer])
                if k:
                    mix_send[p, k] = mixed.astype(BF16)
                    each = copy(
                        5 + PIECES + p, k, mix_send.at[p, k], mix_recv.at[p, k], {"ch": peer}
                    )
                    each.start()
                    results.append(each)
                else:
                    mix_recv[p, 0] = mixed.astype(BF16)
        for p in range(PIECES):
            for each in tokens[p].values():
                each.wait_send()
        finish(results)
        for p in range(PIECES):
            for h in range(2):
                begin = pl.multiple_of(half_of(h) * half + p * piece, 16)
                mixed = shift[2:3]
                for k in range(h, chans, 2):
                    mixed = mixed + mix_recv[p, k].astype(F32)
                x[pl.ds(begin, piece)] = x[pl.ds(begin, piece)] + mixed

    step(True)

    @pl.loop(1, STEPS)
    def _(_index):
        step(False)

    for r in range(rows):
        out[r] = x[r * padded : r * padded + width]


def block_diagonal(weights):
    parts, blocks, size, _ = weights.shape
    eye = jnp.eye(blocks, dtype=weights.dtype)
    spread = weights[:, :, :, None, :] * eye[None, :, None, :, None]
    return spread.reshape(parts, blocks * size, blocks * size)


def fused(
    lats,
    chans,
    state,
    norm_gains,
    channel_biases,
    filter_in,
    filter_in_bias,
    filter_out,
    filter_out_bias,
    up_weight,
    up_bias,
    down_weight,
):
    _, rows, width, own = state.shape
    padded = -(-width // 32) * 32
    share = 2 * M // lats
    piece = rows * padded // 2 // PIECES
    hid = up_weight.shape[1]
    tables = fourier_tables(width, padded, rows * lats, M, lats)
    down = down_weight.reshape(hid, chans, own).transpose(1, 0, 2)
    args = (
        state[0],
        norm_gains,
        channel_biases,
        block_diagonal(filter_in),
        filter_in_bias.reshape(2, own),
        block_diagonal(filter_out),
        filter_out_bias.reshape(2, own),
        up_weight.reshape(chans, own, hid),
        up_bias.reshape(1, hid),
        down,
    ) + tuple(jnp.asarray(t) for t in tables)
    vmem = pl.BlockSpec(memory_space=pltpu.VMEM)
    spectrum = (lats, rows, share, own)
    result = pl.pallas_call(
        functools.partial(rollout, lats, chans),
        out_shape=jax.ShapeDtypeStruct((rows, width, own), F32),
        in_specs=[vmem] * len(args),
        out_specs=vmem,
        scratch_shapes=[
            pltpu.VMEM((rows * padded, own), F32),
            pltpu.VMEM((2, 8, rows * padded), F32),
            pltpu.VMEM((2, chans, 8, rows * padded), F32),
            pltpu.VMEM(spectrum, BF16),
            pltpu.VMEM(spectrum, BF16),
            pltpu.VMEM(spectrum, BF16),
            pltpu.VMEM(spectrum, BF16),
            pltpu.VMEM((2, PIECES, piece, own), BF16),
            pltpu.VMEM((PIECES, chans, piece, own), BF16),
            pltpu.VMEM((PIECES, chans, piece, own), BF16),
            pltpu.VMEM((PIECES, chans, piece, own), BF16),
            pltpu.VMEM((8, hid), F32),
            pltpu.VMEM((8, hid), F32),
            pltpu.VMEM((chans, own, hid), BF16),
            pltpu.VMEM(down.shape, BF16),
            pltpu.VMEM((2, piece, hid), F32),
            pltpu.VMEM((2, piece, hid), BF16),
            pltpu.VMEM((2, 2, 2, own, own), BF16),
            pltpu.SemaphoreType.DMA((5 + 2 * PIECES, lats + chans)),
            pltpu.SemaphoreType.DMA((5 + 2 * PIECES, lats + chans)),
        ],
        compiler_params=pltpu.CompilerParams(
            collective_id=0, has_side_effects=True, vmem_limit_bytes=48 * 1024 * 1024
        ),
    )(*args)
    return result[None]


def dispatch(sizes, *args):
    lats, chans = sizes["lat"], sizes["ch"]
    aligned = args[0].shape[1] * (-(-args[0].shape[2] // 32)) * 32 % (32 * PIECES) == 0
    if 2 * M // lats % 16 == 0 and chans % 2 == 0 and aligned:
        return fused(lats, chans, *args)
    return local(*args)


def solution(mesh):
    placed = (
        P(None, "lat", None, "ch"),
        P(None, "ch"),
        P(None, "ch"),
        P(None, "ch", None, None),
        P(None, "ch", None),
        P(None, "ch", None, None),
        P(None, "ch", None),
        P(None, "ch"),
        P("ch"),
        P("ch", None),
    )
    return jax.shard_map(
        functools.partial(dispatch, dict(mesh.shape)), mesh=mesh, in_specs=placed, out_specs=P(None, "lat", None, "ch"), check_vma=False
    )
```

```python
import functools
import math

import jax
import jax.numpy as jnp
from jax import lax
import numpy as np
from jax.experimental import pallas as pl
from jax.experimental.pallas import tpu as pltpu
from jax.sharding import PartitionSpec as P

D = 768
M = 64
STEPS = 4


EPS = 1e-05
SHRINK = 0.01
HIGH = lax.Precision.HIGHEST


def longitude_tables(width, modes):
    column = jnp.arange(width, dtype=jnp.int32)[:, None]
    order = jnp.arange(modes, dtype=jnp.int32)[None, :]
    angle = 2.0 * math.pi / width * (column * order % width).astype(jnp.float32)
    doubled = jnp.where(order == 0, 1.0, 2.0).astype(jnp.float32)
    return (jnp.cos(angle), jnp.sin(angle), jnp.cos(angle) * doubled, jnp.sin(angle) * doubled)


def latitude_tables(height):
    column = jnp.arange(height, dtype=jnp.int32)[:, None]
    order = jnp.arange(height, dtype=jnp.int32)[None, :]
    angle = 2.0 * math.pi / height * (column * order % height).astype(jnp.float32)
    return (jnp.cos(angle), jnp.sin(angle))


def layer_norm(values, gain, shift):
    mean = jnp.sum(values, -1, keepdims=True) / values.shape[-1]
    spread = jnp.sum(values * values, -1, keepdims=True) / values.shape[-1] - mean * mean
    return (values - mean) * lax.rsqrt(spread + EPS) * gain + shift


def soft_shrink(values):
    return jnp.where(
        values > SHRINK, values - SHRINK, jnp.where(values < -SHRINK, values + SHRINK, 0.0)
    )


def block_apply(left, matrix):
    return jnp.einsum("bkmnj,nji->bkmni", left, matrix, precision=HIGH)


def spectral_mlp(real_part, imag_part, filter_in, filter_in_bias, filter_out, filter_out_bias):
    shape = real_part.shape
    blocks = filter_in.shape[1]
    size = filter_in.shape[2]
    real_blocks = real_part.reshape(shape[:-1] + (blocks, size))
    imag_blocks = imag_part.reshape(shape[:-1] + (blocks, size))
    first_real = jax.nn.relu(
        block_apply(real_blocks, filter_in[0])
        - block_apply(imag_blocks, filter_in[1])
        + filter_in_bias[0]
    )
    first_imag = jax.nn.relu(
        block_apply(imag_blocks, filter_in[0])
        + block_apply(real_blocks, filter_in[1])
        + filter_in_bias[1]
    )
    second_real = (
        block_apply(first_real, filter_out[0])
        - block_apply(first_imag, filter_out[1])
        + filter_out_bias[0]
    )
    second_imag = (
        block_apply(first_imag, filter_out[0])
        + block_apply(first_real, filter_out[1])
        + filter_out_bias[1]
    )
    return (soft_shrink(second_real).reshape(shape), soft_shrink(second_imag).reshape(shape))


def local(
    state,
    norm_gains,
    channel_biases,
    filter_in,
    filter_in_bias,
    filter_out,
    filter_out_bias,
    up_weight,
    up_bias,
    down_weight,
):
    width = state.shape[2]
    height = state.shape[1] * lax.axis_size("lat")
    scale = 1.0 / math.sqrt(height * width)
    lon_cos, lon_sin, back_cos, back_sin = longitude_tables(width, M)
    lat_cos, lat_sin = latitude_tables(height)
    gains = norm_gains.astype(jnp.float32)
    shifts = channel_biases.astype(jnp.float32)
    full_up, full_gains, full_biases = (
        lax.all_gather(up_weight, "ch", axis=1, tiled=True),
        lax.all_gather(norm_gains, "ch", axis=1, tiled=True),
        lax.all_gather(channel_biases, "ch", axis=1, tiled=True),
    )
    full_down, full_up_bias = (
        lax.all_gather(down_weight, "ch", axis=0, tiled=True),
        lax.all_gather(up_bias, "ch", axis=0, tiled=True),
    )
    wide_gains = full_gains.astype(jnp.float32)
    wide_biases = full_biases.astype(jnp.float32)
    wide_up_bias = full_up_bias.astype(jnp.float32)
    values = state
    for step_index in range(STEPS):
        total, squares = lax.psum(
            (jnp.sum(values, -1, keepdims=True), jnp.sum(values * values, -1, keepdims=True)), "ch"
        )
        mean = total / D
        mean, spread = (mean, squares / D - mean * mean)
        normed = (values - mean) * lax.rsqrt(spread + EPS) * gains[0] + shifts[0]
        real_lon = jnp.einsum("bhwd,wm->bhmd", normed, lon_cos, precision=HIGH)
        imag_lon = -jnp.einsum("bhwd,wm->bhmd", normed, lon_sin, precision=HIGH)
        stacked = lax.all_to_all(
            jnp.stack((real_lon, imag_lon)), "lat", split_axis=3, concat_axis=2, tiled=True
        )
        spectral_real_lon = stacked[0]
        spectral_imag_lon = stacked[1]
        real_spec = (
            jnp.einsum("kh,bhmd->bkmd", lat_cos, spectral_real_lon, precision=HIGH)
            + jnp.einsum("kh,bhmd->bkmd", lat_sin, spectral_imag_lon, precision=HIGH)
        ) * scale
        imag_spec = (
            jnp.einsum("kh,bhmd->bkmd", lat_cos, spectral_imag_lon, precision=HIGH)
            - jnp.einsum("kh,bhmd->bkmd", lat_sin, spectral_real_lon, precision=HIGH)
        ) * scale
        out_real, out_imag = spectral_mlp(
            real_spec, imag_spec, filter_in, filter_in_bias, filter_out, filter_out_bias
        )
        real_rows = jnp.einsum("kh,bkmd->bhmd", lat_cos, out_real, precision=HIGH) - jnp.einsum(
            "kh,bkmd->bhmd", lat_sin, out_imag, precision=HIGH
        )
        imag_rows = jnp.einsum("kh,bkmd->bhmd", lat_cos, out_imag, precision=HIGH) + jnp.einsum(
            "kh,bkmd->bhmd", lat_sin, out_real, precision=HIGH
        )
        rows = lax.all_to_all(
            jnp.stack((real_rows, imag_rows)), "lat", split_axis=2, concat_axis=3, tiled=True
        )
        back = jnp.einsum("bhmd,wm->bhwd", rows[0], back_cos, precision=HIGH) - jnp.einsum(
            "bhmd,wm->bhwd", rows[1], back_sin, precision=HIGH
        )
        values = values + back * scale + normed
        owned = lax.all_to_all(values, "ch", split_axis=2, concat_axis=3, tiled=True)
        normed_two = layer_norm(owned, wide_gains[1], wide_biases[1]).astype(jnp.bfloat16)
        flat = normed_two.reshape(-1, normed_two.shape[-1])
        pre = jnp.dot(flat, full_up, preferred_element_type=jnp.float32) + wide_up_bias
        hidden = jax.nn.gelu(pre, approximate=False).astype(jnp.bfloat16)
        mixed = jnp.dot(hidden, full_down, preferred_element_type=jnp.float32) + wide_biases[2]
        values = values + lax.all_to_all(
            mixed.reshape(owned.shape), "ch", split_axis=3, concat_axis=2, tiled=True
        )
    return values


PIECES = 3
F32 = jnp.float32
BF16 = jnp.bfloat16
MESH = pl.DeviceIdType.MESH


def split_table(table):
    high = np.asarray(table, np.float32).astype(jnp.bfloat16)
    low = (table - high.astype(np.float64)).astype(np.float32).astype(jnp.bfloat16)
    return np.stack((high, low))


def fourier_tables(width, padded, height, modes, owners):
    scale = 1.0 / math.sqrt(height * width)
    share = modes // owners
    order = np.arange(modes).reshape(owners, share)
    angle = 2.0 * np.pi / width * (order[:, :, None] * np.arange(width) % width)
    forward = np.zeros((owners, 2, share, padded))
    forward[:, 0, :, :width] = np.cos(angle)
    forward[:, 1, :, :width] = -np.sin(angle)
    doubled = np.where(order == 0, 1.0, 2.0)[:, None, :, None] * scale
    backward = (forward * doubled).reshape(2 * modes, padded).T
    forward = forward.reshape(2 * modes, padded)
    rows = np.arange(height)
    turn = 2.0 * np.pi / height * (rows[:, None] * rows[None, :] % height)
    cos, sin, eye = np.cos(turn), np.sin(turn), np.eye(share)
    mix = np.array([[cos, sin], [-sin, cos]])
    size = 2 * height * share
    lat = np.einsum("abkh,mn->akmhbn", mix, eye).reshape(size, size) * scale
    unmix = np.array([[cos, -sin], [sin, cos]])
    back = np.einsum("bahk,mn->hbmakn", unmix, eye).reshape(size, size)
    return tuple(split_table(t) for t in (forward, lat, back, backward))


def dot(left, right):
    return jnp.dot(left, right, preferred_element_type=F32)


def halves(values):
    high = values.astype(BF16)
    return high, (values - high.astype(F32)).astype(BF16)


def gelu(values):
    return 0.5 * values * (1.0 + lax.erf(values * (1.0 / math.sqrt(2.0))))


def rollout(
    lats,
    chans,
    state,
    gains,
    shifts,
    fin,
    fin_bias,
    fout,
    fout_bias,
    up,
    up_bias,
    down,
    t_lon,
    t_lat,
    t_rows,
    t_back,
    out,
    x,
    stat_send,
    stat_recv,
    lon_send,
    lon_recv,
    row_send,
    row_recv,
    tok_send,
    tok_recv,
    mix_send,
    mix_recv,
    bias_send,
    bias_recv,
    up_recv,
    down_recv,
    partial,
    hidden,
    mixing,
    send_sem,
    recv_sem,
):
    lat, ch = lax.axis_index("lat"), lax.axis_index("ch")
    core = lax.rem(ch, 2)
    partner = ch + 1 - 2 * core
    rows, width, own = state.shape
    padded = x.shape[0] // rows
    half = x.shape[0] // 2
    piece = half // PIECES
    modes = t_lon.shape[1]
    wide = chans * own
    hid = up.shape[-1]

    def lat_peer(k):
        return lax.rem(lat + k, lats)

    def ch_peer(k):
        return lax.rem((partner if k % 2 else ch) + k - k % 2, chans)

    def ch_source(k):
        return lax.rem((partner if k % 2 else ch) + chans - (k - k % 2), chans)

    def half_of(k):
        return 1 - core if k % 2 else core

    far_first = tuple(range(2, chans)) + (1,)

    barrier = pltpu.get_barrier_semaphore()
    for k in range(1, lats):
        pl.semaphore_signal(barrier, inc=1, device_id={"lat": lat_peer(k)}, device_id_type=MESH)
    for k in range(1, chans):
        pl.semaphore_signal(barrier, inc=1, device_id={"ch": ch_peer(k)}, device_id_type=MESH)

    def copy(kind, k, source, target, device):
        return pltpu.make_async_remote_copy(
            src_ref=source,
            dst_ref=target,
            send_sem=send_sem.at[kind, k],
            recv_sem=recv_sem.at[kind, k],
            device_id=device,
            device_id_type=MESH,
        )

    gain = gains[...].astype(F32)
    shift = shifts[...].astype(F32)
    bias_send[...] = jnp.broadcast_to(up_bias[...].astype(F32), bias_send.shape)
    x[...] = jnp.zeros_like(x)
    for r in range(rows):
        x[r * padded : r * padded + width] = state[r]
    for layer, weights in enumerate((fin, fout)):
        for i in range(2):
            mixing[layer, i, 0], mixing[layer, i, 1] = halves(weights[i])
    pl.semaphore_wait(barrier, lats + chans - 2)
    setup = [
        copy(2, 0, bias_send, bias_recv, {"ch": partner}),
        copy(3, 0, up, up_recv, {"ch": partner}),
        copy(4, 0, down, down_recv, {"ch": partner}),
    ]
    lane = lax.broadcasted_iota(jnp.int32, (x.shape[0], 128), 1)

    def start(copies):
        for each in copies:
            each.start()
        return copies

    def finish(copies):
        for each in copies:
            each.wait()

    def norm_terms(kind, extra):
        values = x[...]
        total = jnp.sum(values, -1, keepdims=True)
        squares = jnp.sum(values * values, -1, keepdims=True)
        packed = jnp.where(lane == 0, total, jnp.where(lane == 1, squares, 0.0))
        stat_send[kind] = jnp.transpose(packed)[0:8]
        copies = start(
            [
                copy(kind, lats + k, stat_send.at[kind], stat_recv.at[kind, k], {"ch": ch_peer(k)})
                for k in range(1, chans)
            ]
        )
        start(extra)
        finish(copies)
        total = stat_send[kind]
        for k in range(1, chans):
            total = total + stat_recv[kind, k]
        total = jnp.transpose(total)
        mean = total[:, 0:1] / wide
        return mean, lax.rsqrt(total[:, 1:2] / wide - mean * mean + EPS)

    def step(first):
        mean, scaled = norm_terms(0, setup if first else [])
        for r in range(rows):
            part = slice(r * padded, (r + 1) * padded)
            now = x[part]
            normed = (now - mean[part]) * scaled[part] * gain[0:1] + shift[0:1]
            x[part] = now + normed
            high, low = halves(normed)
            spectra = dot(t_lon[0], high) + dot(t_lon[0], low) + dot(t_lon[1], high)
            lon_send[:, r] = spectra.astype(BF16).reshape(lats, modes // lats, own)
        copies = start(
            [
                copy(0, k, lon_send.at[lat_peer(k)], lon_recv.at[lat], {"lat": lat_peer(k)})
                for k in range(1, lats)
            ]
        )
        lon_recv[pl.ds(lat, 1)] = lon_send[pl.ds(lat, 1)]
        finish(copies)
        data = lon_recv[...].reshape(-1, own)
        spec = dot(t_lat[0], data) + dot(t_lat[1], data)
        split = spec.shape[0] // 2

        def complex_apply(pair, layer, bias):
            high, low = halves(pair)
            one, two = (
                dot(high, mixing[layer, i, 0])
                + dot(low, mixing[layer, i, 0])
                + dot(high, mixing[layer, i, 1])
                for i in range(2)
            )
            return (one[:split] - two[split:] + bias[0:1], one[split:] + two[:split] + bias[1:2])

        real, imag = complex_apply(spec, 0, fin_bias)
        pair = jnp.concatenate((jnp.maximum(real, 0.0), jnp.maximum(imag, 0.0)), 0)
        real, imag = complex_apply(pair, 1, fout_bias)
        high, low = halves(jnp.concatenate((soft_shrink(real), soft_shrink(imag)), 0))
        back = dot(t_rows[0], high) + dot(t_rows[0], low) + dot(t_rows[1], high)
        row_send[...] = back.astype(BF16).reshape(row_send.shape)
        copies = start(
            [
                copy(1, k, row_send.at[lat_peer(k)], row_recv.at[lat], {"lat": lat_peer(k)})
                for k in range(1, lats)
            ]
        )
        row_recv[pl.ds(lat, 1)] = row_send[pl.ds(lat, 1)]
        finish(copies)
        for r in range(rows):
            part = slice(r * padded, (r + 1) * padded)
            data = row_recv[:, r].reshape(-1, own)
            x[part] = x[part] + dot(t_back[0], data) + dot(t_back[1], data)
        mean, scaled = norm_terms(1, [])
        for p in range(PIECES):
            for h in range(2):
                part = slice(h * half + p * piece, h * half + (p + 1) * piece)
                normed = (x[part] - mean[part]) * scaled[part] * gain[1:2] + shift[1:2]
                tok_send[h, p] = normed.astype(BF16)
        tokens = [
            {
                k: copy(
                    5 + p, k, tok_send.at[half_of(k), p], tok_recv.at[p, k], {"ch": ch_peer(k)}
                )
                for k in far_first
            }
            for p in range(PIECES)
        ]
        for p in range(PIECES):
            start(tokens[p].values())
        if first:
            finish(setup)
        results = []
        chunk = 256
        blocks = [(s, lo) for s in range(2) for lo in range(0, hid, chunk)]
        for p in range(PIECES):
            tok_recv[p, 0] = tok_send[core, p]
            tokens[p][1].wait_recv()
            for s, lo in blocks:
                weight, bias = ((up, bias_send), (up_recv, bias_recv))[s]
                cut = slice(lo, lo + chunk)
                pre = bias[0:1, cut]
                for k in range(2):
                    pre = pre + dot(tok_recv[p, k], weight[ch_source(k), :, cut])
                partial[s, :, cut] = pre
            for k in range(2, chans):
                tokens[p][k].wait_recv()
            for s, lo in blocks:
                weight = (up, up_recv)[s]
                cut = slice(lo, lo + chunk)
                pre = partial[s, :, cut]
                for k in range(2, chans):
                    pre = pre + dot(tok_recv[p, k], weight[ch_source(k), :, cut])
                hidden[s, :, cut] = gelu(pre).astype(BF16)
            for k in far_first + (0,):
                peer = ch_peer(k)
                mixed = dot(hidden[0], down[peer]) + dot(hidden[1], down_recv[peer])
                if k:
                    mix_send[p, k] = mixed.astype(BF16)
                    each = copy(
                        5 + PIECES + p, k, mix_send.at[p, k], mix_recv.at[p, k], {"ch": peer}
                    )
                    each.start()
                    results.append(each)
                else:
                    mix_recv[p, 0] = mixed.astype(BF16)
        for p in range(PIECES):
            for each in tokens[p].values():
                each.wait_send()
        finish(results)
        for p in range(PIECES):
            for h in range(2):
                begin = pl.multiple_of(half_of(h) * half + p * piece, 16)
                mixed = shift[2:3]
                for k in range(h, chans, 2):
                    mixed = mixed + mix_recv[p, k].astype(F32)
                x[pl.ds(begin, piece)] = x[pl.ds(begin, piece)] + mixed

    step(True)

    @pl.loop(1, STEPS)
    def _(_index):
        step(False)

    for r in range(rows):
        out[r] = x[r * padded : r * padded + width]


def block_diagonal(weights):
    parts, blocks, size, _ = weights.shape
    eye = jnp.eye(blocks, dtype=weights.dtype)
    spread = weights[:, :, :, None, :] * eye[None, :, None, :, None]
    return spread.reshape(parts, blocks * size, blocks * size)


def fused(
    lats,
    chans,
    state,
    norm_gains,
    channel_biases,
    filter_in,
    filter_in_bias,
    filter_out,
    filter_out_bias,
    up_weight,
    up_bias,
    down_weight,
):
    _, rows, width, own = state.shape
    padded = -(-width // 32) * 32
    share = 2 * M // lats
    piece = rows * padded // 2 // PIECES
    hid = up_weight.shape[1]
    tables = fourier_tables(width, padded, rows * lats, M, lats)
    down = down_weight.reshape(hid, chans, own).transpose(1, 0, 2)
    args = (
        state[0],
        norm_gains,
        channel_biases,
        block_diagonal(filter_in),
        filter_in_bias.reshape(2, own),
        block_diagonal(filter_out),
        filter_out_bias.reshape(2, own),
        up_weight.reshape(chans, own, hid),
        up_bias.reshape(1, hid),
        down,
    ) + tuple(jnp.asarray(t) for t in tables)
    vmem = pl.BlockSpec(memory_space=pltpu.VMEM)
    spectrum = (lats, rows, share, own)
    result = pl.pallas_call(
        functools.partial(rollout, lats, chans),
        out_shape=jax.ShapeDtypeStruct((rows, width, own), F32),
        in_specs=[vmem] * len(args),
        out_specs=vmem,
        scratch_shapes=[
            pltpu.VMEM((rows * padded, own), F32),
            pltpu.VMEM((2, 8, rows * padded), F32),
            pltpu.VMEM((2, chans, 8, rows * padded), F32),
            pltpu.VMEM(spectrum, BF16),
            pltpu.VMEM(spectrum, BF16),
            pltpu.VMEM(spectrum, BF16),
            pltpu.VMEM(spectrum, BF16),
            pltpu.VMEM((2, PIECES, piece, own), BF16),
            pltpu.VMEM((PIECES, chans, piece, own), BF16),
            pltpu.VMEM((PIECES, chans, piece, own), BF16),
            pltpu.VMEM((PIECES, chans, piece, own), BF16),
            pltpu.VMEM((8, hid), F32),
            pltpu.VMEM((8, hid), F32),
            pltpu.VMEM((chans, own, hid), BF16),
            pltpu.VMEM(down.shape, BF16),
            pltpu.VMEM((2, piece, hid), F32),
            pltpu.VMEM((2, piece, hid), BF16),
            pltpu.VMEM((2, 2, 2, own, own), BF16),
            pltpu.SemaphoreType.DMA((5 + 2 * PIECES, lats + chans)),
            pltpu.SemaphoreType.DMA((5 + 2 * PIECES, lats + chans)),
        ],
        compiler_params=pltpu.CompilerParams(
            collective_id=0, has_side_effects=True, vmem_limit_bytes=48 * 1024 * 1024
        ),
    )(*args)
    return result[None]


def dispatch(sizes, *args):
    lats, chans = sizes["lat"], sizes["ch"]
    aligned = args[0].shape[1] * (-(-args[0].shape[2] // 32)) * 32 % (32 * PIECES) == 0
    if 2 * M // lats % 16 == 0 and chans % 2 == 0 and aligned:
        return fused(lats, chans, *args)
    return local(*args)


def solution(mesh):
    placed = (
        P(None, "lat", None, "ch"),
        P(None, "ch"),
        P(None, "ch"),
        P(None, "ch", None, None),
        P(None, "ch", None),
        P(None, "ch", None, None),
        P(None, "ch", None),
        P(None, "ch"),
        P("ch"),
        P("ch", None),
    )
    return jax.shard_map(
        functools.partial(dispatch, dict(mesh.shape)), mesh=mesh, in_specs=placed, out_specs=P(None, "lat", None, "ch"), check_vma=False
    )
```
